32 devices in a mesh: tile: 8 (over z, x), cls: 4 (over y, core).
Axes of the slice: x: 2, y: 2, z: 4, core: 2. Of those that a mesh axis runs over, the one named last changes fastest.
Arguments:
- concentration: float32 [64, 4, 16384], P('cls', None, 'tile'), may hold values from 0.05 to 2
- velocity: float32 [2, 4, 16384], P(None, None, 'tile'), may hold values from -0.3 to 0.3
- land_mask: int32 [16384], P('tile'), may hold values 0 or 1
- settling: float32 [64], P('cls'), may hold values from 0.01 to 0.3
- breakage_rate: float32 [64], replicated, may hold values from 0.02 to 0.3
- kernel_levels: int32 [64, 64], replicated, may hold values from 100 to 1000, as said below
- pair_target: int32 [64, 64], replicated, may hold values from 0 to 63, as said below
- fragment_weights: int32 [64, 64], replicated, may hold values from 1 to 16
Outputs:
- flocs: float32 [64, 4, 16384], P('cls', None, 'tile')
The draws below stay inside these ranges and needn't reach their ends.
Inputs may be any that keep to these rules, and one draw needn't show every extreme that they name: `kernel_levels`: symmetric. `pair_target`: symmetric, and entry [i, j] is at least the larger of i and j.
All inputs are finite; a program needn't handle non-finite values. No bound on the sum of `land_mask` on one device may be relied on, other than what follows from the above.
Results may differ from the reference program's by a relative error of at most 0.0001.
Values sent between devices are 32-bit elements; how exact they have to be, the bound alone decides.
A program may use at most 64 MiB of HBM per device.

```python
import math
import jax
import jax.numpy as jnp
from jax import lax

NC = 64
L = 4
CY = 512
CX = 4
COLUMNS = 16384
N_TILE = 8


def draw_kernel_levels(key, part):
    half = jax.random.randint(jax.random.fold_in(key, 11), (NC, NC), 50, 501, dtype=jnp.int32)
    return (half + half.T).astype(jnp.int32)


def draw_pair_target(key, part):
    extra = jax.random.randint(jax.random.fold_in(key, 23), (NC, NC), 0, 2, dtype=jnp.int32)
    extra = extra + extra.T
    rank = jnp.arange(NC, dtype=jnp.int32)
    larger = jnp.maximum(rank[:, None], rank[None, :])
    return jnp.minimum(larger + extra, NC - 1).astype(jnp.int32)


def plant(values, key, low, top_value):
    index_at = [jax.random.randint(jax.random.fold_in(key, axis), (), 0, length) for axis, length in enumerate(values.shape)]
    longest = values.shape.index(max(values.shape))
    next_to = index_at[:longest] + [(index_at[longest] + 1) % values.shape[longest]] + index_at[longest + 1:]
    return values.at[tuple(index_at)].set(low).at[tuple(next_to)].set(top_value)


def block_levels(rng, dims, cuts, least, largest):
    loudness = 1.0
    for position, shards_of in cuts:
        heights = jax.random.uniform(jax.random.fold_in(jax.random.fold_in(rng, 6), position), (shards_of,), jnp.float32, least / len(cuts), largest / len(cuts))
        loudness = loudness * jnp.repeat(jnp.exp(heights), dims[position] // shards_of).reshape((-1,) + (1,) * (len(dims) - 1 - position))
    return loudness


def setup_inputs(seed: int = 0) -> dict:
    key_of = jax.random.split(jax.random.key(seed), 9)
    concentration = jnp.clip(jnp.exp(math.log(2.0) - 3.6888794 * jax.random.uniform(key_of[0], (NC, L, COLUMNS), jnp.float32) ** block_levels(key_of[0], (NC, L, COLUMNS), ((0, 4), (2, 8)), -0.2, 0.2)), 0.05, 2.0)
    velocity = jnp.clip(jax.random.uniform(key_of[1], (2, L, COLUMNS), jnp.float32, -0.3, 0.3) * block_levels(key_of[1], (2, L, COLUMNS), ((2, 8),), -0.4, 0.0), -0.3, 0.3)
    land_mask = plant((jax.random.randint(key_of[2], (COLUMNS,), 0, 8) < 7).astype(jnp.int32), jax.random.fold_in(key_of[2], 1), 0, 1)
    settling = jnp.clip(jnp.exp(math.log(0.3) - 3.4011974 * jax.random.uniform(key_of[3], (NC,), jnp.float32) ** block_levels(key_of[3], (NC,), ((0, 4),), -0.2, 0.2)), 0.01, 0.3)
    breakage_rate = jnp.clip(jnp.exp(jax.random.uniform(key_of[4], (NC,), jnp.float32, math.log(0.02), math.log(0.3))), 0.02, 0.3)
    kernel_levels = draw_kernel_levels(jax.random.fold_in(key_of[8], 71), 0)
    pair_target = draw_pair_target(jax.random.fold_in(key_of[8], 71), 0)
    fragment_weights = plant(jax.random.randint(key_of[7], (NC, NC), 1, 17), jax.random.fold_in(key_of[7], 1), 1, 16).astype(jnp.int32)
    return dict(concentration=concentration, velocity=velocity, land_mask=land_mask, settling=settling, breakage_rate=breakage_rate, kernel_levels=kernel_levels, pair_target=pair_target, fragment_weights=fragment_weights)


kernel_scale = 1e-5


def to_grid(array):
    lead = array.shape[:-1]
    return array.reshape(lead + (N_TILE * CX, CY))


def from_grid(array):
    lead = array.shape[:-2]
    return array.reshape(lead + (N_TILE * CX * CY,))


def face_flux(c_low, c_high, f_low, f_high, w_low, w_high):
    speed = 0.5 * (f_low + f_high) * w_low * w_high
    return jnp.maximum(speed, 0.0) * c_low + jnp.minimum(speed, 0.0) * c_high


def reference(concentration, velocity, land_mask, settling, breakage_rate, kernel_levels, pair_target, fragment_weights):
    field = to_grid(concentration)
    speeds = to_grid(velocity)
    water = to_grid(land_mask.astype(jnp.float32))
    cpad = jnp.pad(field, ((0, 0), (0, 0), (1, 1), (1, 1)))
    spad = jnp.pad(speeds, ((0, 0), (0, 0), (1, 1), (1, 1)))
    wpad = jnp.pad(water, ((1, 1), (1, 1)))
    fx = face_flux(cpad[:, :, :-1, 1:-1], cpad[:, :, 1:, 1:-1], spad[0, :, :-1, 1:-1], spad[0, :, 1:, 1:-1], wpad[:-1, 1:-1], wpad[1:, 1:-1])
    fy = face_flux(cpad[:, :, 1:-1, :-1], cpad[:, :, 1:-1, 1:], spad[1, :, 1:-1, :-1], spad[1, :, 1:-1, 1:], wpad[1:-1, :-1], wpad[1:-1, 1:])
    moved = field - (fx[:, :, 1:] - fx[:, :, :-1]) - (fy[:, :, :, 1:] - fy[:, :, :, :-1])
    sink = settling[:, None, None, None] * field
    moved = moved - sink + jnp.pad(sink[:, :-1], ((0, 0), (1, 0), (0, 0), (0, 0)))
    current = from_grid(moved).reshape(NC, -1)

    levels = kernel_levels.astype(jnp.float32) * kernel_scale
    rank = jnp.arange(NC, dtype=jnp.int32)
    hit = pair_target[None, :, :] == rank[:, None, None]
    birth = jnp.where(hit, 0.5 * levels[None, :, :], 0.0)
    lower = jnp.where(rank[:, None] <= rank[None, :], fragment_weights.astype(jnp.float32), 0.0)
    frag = lower / jnp.sum(lower, axis=0, keepdims=True)
    by_first = jnp.transpose(birth, (1, 0, 2))
    for sub in range(2):
        def add_pair(total, item):
            table, partner = item
            made = jnp.dot(table, current, precision=lax.Precision.HIGHEST, preferred_element_type=jnp.float32)
            return total + made * partner[None, :], None
        gain, _ = lax.scan(add_pair, jnp.zeros_like(current), (by_first, current))
        loss = current * jnp.dot(levels, current, precision=lax.Precision.HIGHEST, preferred_element_type=jnp.float32)
        broken = jnp.dot(frag, breakage_rate[:, None] * current, precision=lax.Precision.HIGHEST, preferred_element_type=jnp.float32) - breakage_rate[:, None] * current
        current = current + gain - loss + broken
    return current.reshape(NC, L, N_TILE * CX * CY)
```

```python
import jax
import jax.numpy as jnp
from jax import lax
from jax.experimental import pallas as pl
from jax.experimental.pallas import tpu as pltpu
from jax.sharding import PartitionSpec as P

CY = 512
CX = 4
half_scale = 0.5e-05
STEP = 16


def passed_along(x, axis, by):
    length = lax.axis_size(axis)
    pairs = [(i, i + by) for i in range(length) if 0 <= i + by < length]
    return lax.ppermute(x, axis, pairs)


def face_flux(low, high, group, part):
    speed = 0.5 * (low[group + part] + high[group + part]) * low[group + 2] * high[group + 2]
    return jnp.maximum(speed, 0.0) * low[:group] + jnp.minimum(speed, 0.0) * high[:group]


def split_pair(value, lane, total):
    high = value.astype(jnp.bfloat16).astype(jnp.float32)
    return jnp.where(lane < total, high, value - high).astype(jnp.bfloat16)


def quad_rows(total):
    return sum(STEP * (total - first) for first in range(0, total, STEP))


def build_tables(levels_ref, target_ref, weights_ref, rate_ref, quad_ref, lin_ref):
    total = levels_ref.shape[0]
    wide = 2 * total
    levels = levels_ref[...].astype(jnp.float32)
    levels = jnp.concatenate([levels, levels], 1)
    target = target_ref[...]
    target = jnp.concatenate([target, target], 1)
    row = lax.broadcasted_iota(jnp.int32, (total, wide), 0)
    lane = lax.broadcasted_iota(jnp.int32, (total, wide), 1)
    col = jnp.where(lane < total, lane, lane - total)
    twice = 2.0 * levels
    birth = jnp.where(col < row, twice, jnp.where(col == row, levels, 0.0))
    offset = 0
    for first in range(0, total, STEP):
        count = total - first
        rank = row[first:]
        for i in range(first, first + STEP):
            value = jnp.where(target[i : i + 1] == rank, birth[i : i + 1], 0.0)
            value = value - jnp.where(rank == i, twice[i : i + 1], 0.0)
            packed = split_pair(value, lane[first:], total)
            quad_ref[offset : offset + count, :wide] = packed
            quad_ref[offset : offset + count, wide:] = packed
            offset += count
    weights = weights_ref[...].astype(jnp.float32)
    weights = jnp.concatenate([weights, weights], 1)
    rate = rate_ref[...]
    rate = jnp.concatenate([rate, rate], 1)
    lower = jnp.where(row <= col, weights, 0.0)
    frag = lower / jnp.sum(lower, axis=0, keepdims=True)
    value = frag * rate - jnp.where(row == col, rate, 0.0)
    packed = split_pair(value, lane, total)
    lin_ref[:, :wide] = packed
    lin_ref[:, wide:] = packed


def react(now, quad_ref, lin_ref):
    total = now.shape[0]
    high = now.astype(jnp.bfloat16)
    low = (now - high.astype(jnp.float32)).astype(jnp.bfloat16)
    stack = jnp.concatenate([high, high, low, low], 0)
    lin = jnp.dot(lin_ref[...], stack, preferred_element_type=jnp.float32)
    gain = None
    offset = 0
    for first in range(0, total, STEP):
        count = total - first
        made = jnp.dot(
            quad_ref[offset : offset + STEP * count, :], stack, preferred_element_type=jnp.float32
        )
        part = made[:count] * now[first : first + 1]
        for r in range(1, STEP):
            part = part + made[r * count : (r + 1) * count] * now[first + r : first + r + 1]
        gain = part if gain is None else jnp.concatenate([gain[:first], gain[first:] + part], 0)
        offset += STEP * count
    return now + gain * half_scale + lin


def react_kernel(chunk, levels_ref, target_ref, weights_ref, rate_ref, whole_ref, out_ref, quad_ref, lin_ref):
    build_tables(levels_ref, target_ref, weights_ref, rate_ref, quad_ref, lin_ref)

    def step(index, carry):
        at = pl.ds(pl.multiple_of(index * chunk, chunk), chunk)
        now = react(whole_ref[:, at], quad_ref, lin_ref)
        out_ref[:, at] = react(now, quad_ref, lin_ref)
        return carry

    lax.fori_loop(0, whole_ref.shape[1] // chunk, step, 0)


def react_all(whole, breakage_rate, kernel_levels, pair_target, fragment_weights):
    total, width = whole.shape
    vmem = pl.BlockSpec(memory_space=pltpu.VMEM)
    import functools

    return pl.pallas_call(
        functools.partial(react_kernel, 256),
        out_shape=jax.ShapeDtypeStruct(whole.shape, jnp.float32),
        in_specs=[vmem] * 5,
        out_specs=vmem,
        scratch_shapes=[
            pltpu.VMEM((quad_rows(total), 4 * total), jnp.bfloat16),
            pltpu.VMEM((total, 4 * total), jnp.bfloat16),
        ],
    )(kernel_levels, pair_target, fragment_weights, breakage_rate.reshape(1, total), whole)


def body(
    concentration,
    velocity,
    land_mask,
    settling,
    breakage_rate,
    kernel_levels,
    pair_target,
    fragment_weights,
):
    group, layers, columns = concentration.shape
    field = concentration.reshape(group, layers, CX, CY)
    water = land_mask.astype(jnp.float32).reshape(1, 1, CX, CY)
    stacked = jnp.concatenate(
        [field, velocity.reshape(2, layers, CX, CY), jnp.broadcast_to(water, (1, layers, CX, CY))],
        0,
    )
    west = passed_along(stacked[:, :, CX - 1 :, :], "tile", 1)
    east = passed_along(stacked[:, :, :1, :], "tile", -1)
    along_x = jnp.concatenate([west, stacked, east], 2)
    along_y = jnp.pad(stacked, ((0, 0), (0, 0), (0, 0), (1, 1)))
    flux_x = face_flux(along_x[:, :, :-1], along_x[:, :, 1:], group, 0)
    flux_y = face_flux(along_y[:, :, :, :-1], along_y[:, :, :, 1:], group, 1)
    moved = (
        field
        - (flux_x[:, :, 1:] - flux_x[:, :, :-1])
        - (flux_y[:, :, :, 1:] - flux_y[:, :, :, :-1])
    )
    sink = settling[:, None, None, None] * field
    moved = moved - sink + jnp.pad(sink[:, :-1], ((0, 0), (1, 0), (0, 0), (0, 0)))
    current = moved.reshape(group, layers, columns)
    whole = lax.all_to_all(current, "cls", 1, 0, tiled=True)
    shape = whole.shape
    done = react_all(
        whole.reshape(shape[0], -1), breakage_rate, kernel_levels, pair_target, fragment_weights
    )
    return lax.all_to_all(done.reshape(shape), "cls", 0, 1, tiled=True)


def solution(mesh):
    return jax.shard_map(
        body,
        mesh=mesh,
        in_specs=(
            P("cls", None, "tile"),
            P(None, None, "tile"),
            P("tile"),
            P("cls"),
            P(),
            P(),
            P(),
            P(),
        ),
        out_specs=P("cls", None, "tile"),
        check_vma=False,
    )
```

```python
import functools

import jax
import jax.numpy as jnp
from jax import lax
from jax.experimental import pallas as pl
from jax.experimental.pallas import tpu as pltpu
from jax.sharding import PartitionSpec as P

CY = 512
CX = 4
half_scale = 0.5e-05
STEP = 16


def split_pair(value, lane, total):
    high = value.astype(jnp.bfloat16).astype(jnp.float32)
    return jnp.where(lane < total, high, value - high).astype(jnp.bfloat16)


def quad_rows(total):
    return sum(STEP * (total - first) for first in range(0, total, STEP))


def build_tables(levels_ref, target_ref, weights_ref, rate_ref, quad_ref, lin_ref):
    total = levels_ref.shape[0]
    wide = 2 * total
    levels = levels_ref[...].astype(jnp.float32)
    levels = jnp.concatenate([levels, levels], 1)
    target = target_ref[...]
    target = jnp.concatenate([target, target], 1)
    row = lax.broadcasted_iota(jnp.int32, (total, wide), 0)
    lane = lax.broadcasted_iota(jnp.int32, (total, wide), 1)
    col = jnp.where(lane < total, lane, lane - total)
    twice = 2.0 * levels
    birth = jnp.where(col < row, twice, jnp.where(col == row, levels, 0.0))
    offset = 0
    for first in range(0, total, STEP):
        count = total - first
        rank = row[first:]
        for i in range(first, first + STEP):
            value = jnp.where(target[i : i + 1] == rank, birth[i : i + 1], 0.0)
            value = value - jnp.where(rank == i, twice[i : i + 1], 0.0)
            packed = split_pair(value, lane[first:], total)
            quad_ref[offset : offset + count, :wide] = packed
            quad_ref[offset : offset + count, wide:] = packed
            offset += count
    weights = weights_ref[...].astype(jnp.float32)
    weights = jnp.concatenate([weights, weights], 1)
    rate = rate_ref[...]
    rate = jnp.concatenate([rate, rate], 1)
    lower = jnp.where(row <= col, weights, 0.0)
    frag = lower / jnp.sum(lower, axis=0, keepdims=True)
    value = frag * rate - jnp.where(row == col, rate, 0.0)
    packed = split_pair(value, lane, total)
    lin_ref[:, :wide] = packed
    lin_ref[:, wide:] = packed


def react(now, quad_ref, lin_ref):
    total = now.shape[0]
    high = now.astype(jnp.bfloat16)
    low = (now - high.astype(jnp.float32)).astype(jnp.bfloat16)
    stack = jnp.concatenate([high, high, low, low], 0)
    lin = jnp.dot(lin_ref[...], stack, preferred_element_type=jnp.float32)
    gain = None
    offset = 0
    for first in range(0, total, STEP):
        count = total - first
        made = jnp.dot(
            quad_ref[offset : offset + STEP * count, :], stack, preferred_element_type=jnp.float32
        )
        part = made[:count] * now[first : first + 1]
        for r in range(1, STEP):
            part = part + made[r * count : (r + 1) * count] * now[first + r : first + r + 1]
        gain = part if gain is None else jnp.concatenate([gain[:first], gain[first:] + part], 0)
        offset += STEP * count
    return now + gain * half_scale + lin


MESH = pl.DeviceIdType.MESH


def step_kernel(
    tiles,
    peers,
    conc_ref,
    speed_ref,
    water_ref,
    settling_ref,
    rate_ref,
    levels_ref,
    target_ref,
    weights_ref,
    out_ref,
    quad_ref,
    lin_ref,
    moved_ref,
    whole_ref,
    done_ref,
    halo_c,
    halo_u,
    halo_w,
    halo_send,
    halo_recv,
    out_send,
    out_recv,
    back_send,
    back_recv,
):
    layers, group, _ = conc_ref.shape
    own = layers // peers
    tile = lax.axis_index("tile")
    me = lax.axis_index("cls")
    has_west = tile > 0
    has_east = tile < tiles - 1

    barrier = pltpu.get_barrier_semaphore()
    for d in range(1, peers):
        pl.semaphore_signal(
            barrier, inc=1, device_id={"cls": lax.rem(me + d, peers)}, device_id_type=MESH
        )

    @pl.when(has_west)
    def _():
        pl.semaphore_signal(barrier, inc=1, device_id={"tile": tile - 1}, device_id_type=MESH)

    @pl.when(has_east)
    def _():
        pl.semaphore_signal(barrier, inc=1, device_id={"tile": tile + 1}, device_id_type=MESH)

    build_tables(levels_ref, target_ref, weights_ref, rate_ref, quad_ref, lin_ref)

    before = lax.div(tile + tiles - 1, tiles)
    after = lax.div(2 * (tiles - 1) - tile, tiles)
    pl.semaphore_wait(barrier, peers - 1 + before + after)

    def cols(x):
        return pl.ds(pl.multiple_of(x * CY, CY), CY)

    def halo(side):
        at = cols(0 if side == 0 else CX - 1)
        to = 1 - side
        where = tile - 1 if side == 0 else tile + 1
        parts = (
            (speed_ref.at[0, :, at], halo_u.at[to]),
            (water_ref.at[:, at], halo_w.at[to]),
            (conc_ref.at[:, :, at], halo_c.at[to]),
        )
        return [
            pltpu.make_async_remote_copy(
                src_ref=part,
                dst_ref=place,
                send_sem=halo_send.at[side, n],
                recv_sem=halo_recv.at[to, n],
                device_id={"tile": where},
                device_id_type=MESH,
            )
            for n, (part, place) in enumerate(parts)
        ]

    def taken(side):
        at = cols(0)
        parts = (
            (speed_ref.at[0, :, at], halo_u.at[side]),
            (water_ref.at[:, at], halo_w.at[side]),
            (conc_ref.at[:, :, at], halo_c.at[side]),
        )
        where = tile - 1 if side == 0 else tile + 1
        return [
            pltpu.make_async_remote_copy(
                src_ref=part,
                dst_ref=place,
                send_sem=halo_send.at[side, n],
                recv_sem=halo_recv.at[side, n],
                device_id={"tile": where},
                device_id_type=MESH,
            )
            for n, (part, place) in enumerate(parts)
        ]

    for side, there in ((0, has_west), (1, has_east)):

        @pl.when(there)
        def _():
            for copy in halo(side):
                copy.start()

        @pl.when(jnp.logical_not(there))
        def _():
            halo_c[side] = jnp.zeros(halo_c.shape[1:], jnp.float32)
            halo_u[side] = jnp.zeros(halo_u.shape[1:], jnp.float32)
            halo_w[side] = jnp.zeros(halo_w.shape[1:], jnp.int32)

    def forward(d, x, s):
        p = lax.rem(me + d, peers)
        return pltpu.make_async_remote_copy(
            src_ref=moved_ref.at[p * own + s, :, cols(x)],
            dst_ref=whole_ref.at[s, pl.ds(pl.multiple_of(me * group, group), group), cols(x)],
            send_sem=out_send.at[d - 1, x, s],
            recv_sem=out_recv.at[d - 1, x, s],
            device_id={"cls": p},
            device_id_type=MESH,
        )

    def backward(d, x, s):
        p = lax.rem(me + d, peers)
        return pltpu.make_async_remote_copy(
            src_ref=done_ref.at[s, pl.ds(pl.multiple_of(p * group, group), group), cols(x)],
            dst_ref=out_ref.at[me * own + s, :, cols(x)],
            send_sem=back_send.at[d - 1, x, s],
            recv_sem=back_recv.at[d - 1, x, s],
            device_id={"cls": p},
            device_id_type=MESH,
        )

    def row_of(x):
        at = cols(x)
        return speed_ref[0, :, at], water_ref[:, at].astype(jnp.float32)

    def halo_row(side):
        return halo_u[side], halo_w[side].astype(jnp.float32)

    def transport(x):
        at = cols(x)
        u, w = row_of(x)
        u_low, w_low = row_of(x - 1) if x > 0 else halo_row(0)
        u_high, w_high = row_of(x + 1) if x < CX - 1 else halo_row(1)
        face_low = 0.5 * (u_low + u) * (w_low * w)
        face_high = 0.5 * (u + u_high) * (w * w_high)
        v = speed_ref[1, :, at]
        lane = lax.broadcasted_iota(jnp.int32, v.shape, 1)
        w_full = jnp.broadcast_to(w, v.shape)
        side_high = 0.5 * (v + pltpu.roll(v, CY - 1, 1)) * (w_full * pltpu.roll(w_full, CY - 1, 1))
        side_high = jnp.where(lane == CY - 1, 0.0, side_high)
        side_low = pltpu.roll(side_high, 1, 1)
        up = jnp.maximum
        down = jnp.minimum
        centre = (
            1.0 - up(face_high, 0.0) + down(face_low, 0.0) - up(side_high, 0.0) + down(side_low, 0.0)
        )
        west = up(face_low, 0.0)
        east = -down(face_high, 0.0)
        south = up(side_low, 0.0)
        north = -down(side_high, 0.0)
        settle = jnp.broadcast_to(settling_ref[...], (group, CY))
        for l in range(layers):
            c = conc_ref[l, :, at]
            c_west = conc_ref[l, :, cols(x - 1)] if x > 0 else halo_c[0, l]
            c_east = conc_ref[l, :, cols(x + 1)] if x < CX - 1 else halo_c[1, l]
            moved = (
                (centre[l : l + 1] - settle) * c
                + west[l : l + 1] * c_west
                + east[l : l + 1] * c_east
                + south[l : l + 1] * pltpu.roll(c, 1, 1)
                + north[l : l + 1] * pltpu.roll(c, CY - 1, 1)
            )
            if l > 0:
                moved = moved + settle * conc_ref[l - 1, :, at]
            moved_ref[l, :, at] = moved
        for s in range(own):
            whole_ref[s, pl.ds(pl.multiple_of(me * group, group), group), at] = moved_ref[
                me * own + s, :, at
            ]
        for s in range(own):
            for d in range(1, peers):
                forward(d, x, s).start()

    for x in range(1, CX - 1):
        transport(x)
    for side, there, x in ((1, has_east, CX - 1), (0, has_west, 0)):

        @pl.when(there)
        def _():
            for copy in taken(side):
                copy.wait_recv()

        transport(x)

    half = CY // 2

    def react_row(q, carry):
        x = lax.rem(q + 1, CX)
        for s in range(own):
            for d in range(1, peers):
                forward(d, x, s).wait_recv()

            def part(h, carry):
                at = pl.ds(pl.multiple_of(x * CY + h * half, half), half)
                now = react(whole_ref[s, :, at], quad_ref, lin_ref)
                done_ref[s, :, at] = react(now, quad_ref, lin_ref)
                return carry

            lax.fori_loop(0, 2, part, 0)
            out_ref[me * own + s, :, cols(x)] = done_ref[
                s, pl.ds(pl.multiple_of(me * group, group), group), cols(x)
            ]
            for d in range(1, peers):
                backward(d, x, s).start()
        return carry

    lax.fori_loop(0, CX, react_row, 0)

    for side, there in ((0, has_west), (1, has_east)):

        @pl.when(there)
        def _():
            for copy in halo(side):
                copy.wait_send()

    def finish(x, carry):
        for s in range(own):
            for d in range(1, peers):
                forward(d, x, s).wait_send()
                copy = backward(d, x, s)
                copy.wait_send()
                copy.wait_recv()
        return carry

    lax.fori_loop(0, CX, finish, 0)


def body(
    tiles,
    peers,
    concentration,
    velocity,
    land_mask,
    settling,
    breakage_rate,
    kernel_levels,
    pair_target,
    fragment_weights,
):
    group, layers, columns = concentration.shape
    total = kernel_levels.shape[0]
    own = layers // peers
    vmem = pl.BlockSpec(memory_space=pltpu.VMEM)
    dma = pltpu.SemaphoreType.DMA
    done = pl.pallas_call(
        functools.partial(step_kernel, tiles, peers),
        out_shape=jax.ShapeDtypeStruct((layers, group, columns), jnp.float32),
        in_specs=[vmem] * 8,
        out_specs=vmem,
        scratch_shapes=[
            pltpu.VMEM((quad_rows(total), 4 * total), jnp.bfloat16),
            pltpu.VMEM((total, 4 * total), jnp.bfloat16),
            pltpu.VMEM((layers, group, columns), jnp.float32),
            pltpu.VMEM((own, total, columns), jnp.float32),
            pltpu.VMEM((own, total, columns), jnp.float32),
            pltpu.VMEM((2, layers, group, CY), jnp.float32),
            pltpu.VMEM((2, layers, CY), jnp.float32),
            pltpu.VMEM((2, 1, CY), jnp.int32),
            dma((2, 3)),
            dma((2, 3)),
            dma((peers - 1, CX, own)),
            dma((peers - 1, CX, own)),
            dma((peers - 1, CX, own)),
            dma((peers - 1, CX, own)),
        ],
        compiler_params=pltpu.CompilerParams(collective_id=0, has_side_effects=True),
    )(
        jnp.transpose(concentration, (1, 0, 2)),
        velocity,
        land_mask.reshape(1, columns),
        settling.reshape(group, 1),
        breakage_rate.reshape(1, total),
        kernel_levels,
        pair_target,
        fragment_weights,
    )
    return jnp.transpose(done, (1, 0, 2))


def solution(mesh):
    return jax.shard_map(
        functools.partial(body, mesh.shape["tile"], mesh.shape["cls"]),
        mesh=mesh,
        in_specs=(
            P("cls", None, "tile"),
            P(None, None, "tile"),
            P("tile"),
            P("cls"),
            P(),
            P(),
            P(),
            P(),
        ),
        out_specs=P("cls", None, "tile"),
        check_vma=False,
    )
```

```python
import functools

import jax
import jax.numpy as jnp
from jax import lax
from jax.experimental import pallas as pl
from jax.experimental.pallas import tpu as pltpu
from jax.sharding import PartitionSpec as P

CY = 512
CX = 4
half_scale = 0.5e-05
STEP = 16
LANES = 128


def split_pair(value, lane, total):
    high = value.astype(jnp.bfloat16).astype(jnp.float32)
    return jnp.where(lane < total, high, value - high).astype(jnp.bfloat16)


def quad_rows(total):
    return sum(STEP * (total - first) for first in range(0, total, STEP))


def build_tables(levels_ref, target_ref, weights_ref, rate_ref, quad_ref, lin_ref):
    total = levels_ref.shape[0]
    wide = 2 * total
    levels = levels_ref[...].astype(jnp.float32)
    levels = jnp.concatenate([levels, levels], 1)
    target = target_ref[...]
    target = jnp.concatenate([target, target], 1)
    row = lax.broadcasted_iota(jnp.int32, (total, wide), 0)
    lane = lax.broadcasted_iota(jnp.int32, (total, wide), 1)
    col = jnp.where(lane < total, lane, lane - total)
    twice = 2.0 * levels
    birth = jnp.where(col < row, twice, jnp.where(col == row, levels, 0.0))
    offset = 0
    for first in range(0, total, STEP):
        count = total - first
        rank = row[first:]
        for i in range(first, first + STEP):
            value = jnp.where(target[i : i + 1] == rank, birth[i : i + 1], 0.0)
            value = value - jnp.where(rank == i, twice[i : i + 1], 0.0)
            packed = split_pair(value, lane[first:], total)
            quad_ref[offset : offset + count, :wide] = packed
            quad_ref[offset : offset + count, wide:] = packed
            offset += count
    weights = weights_ref[...].astype(jnp.float32)
    weights = jnp.concatenate([weights, weights], 1)
    rate = rate_ref[...]
    rate = jnp.concatenate([rate, rate], 1)
    lower = jnp.where(row <= col, weights, 0.0)
    frag = lower / jnp.sum(lower, axis=0, keepdims=True)
    value = frag * rate - jnp.where(row == col, rate, 0.0)
    packed = split_pair(value, lane, total)
    lin_ref[:, :wide] = packed
    lin_ref[:, wide:] = packed


def react(now, quad_ref, lin_ref):
    total = now.shape[0]
    high = now.astype(jnp.bfloat16)
    low = (now - high.astype(jnp.float32)).astype(jnp.bfloat16)
    stack = jnp.concatenate([high, high, low, low], 0)
    lin = jnp.dot(lin_ref[...], stack, preferred_element_type=jnp.float32)
    gain = None
    offset = 0
    for first in range(0, total, STEP):
        count = total - first
        made = jnp.dot(
            quad_ref[offset : offset + STEP * count, :], stack, preferred_element_type=jnp.float32
        )
        part = made[:count] * now[first : first + 1]
        for r in range(1, STEP):
            part = part + made[r * count : (r + 1) * count] * now[first + r : first + r + 1]
        gain = part if gain is None else jnp.concatenate([gain[:first], gain[first:] + part], 0)
        offset += STEP * count
    return now + gain * half_scale + lin


MESH = pl.DeviceIdType.MESH


def step_kernel(
    tiles,
    peers,
    flat_ref,
    speed_ref,
    water_ref,
    settling_ref,
    rate_ref,
    levels_ref,
    target_ref,
    weights_ref,
    out_ref,
    quad_ref,
    lin_ref,
    conc_ref,
    moved_ref,
    whole_ref,
    done_ref,
    back_ref,
    halo_c,
    halo_u,
    halo_w,
    halo_send,
    halo_recv,
    out_send,
    out_recv,
    back_send,
    back_recv,
):
    layers, group, columns = conc_ref.shape
    tile_lanes = columns // LANES
    own = layers // peers
    tile = lax.axis_index("tile")
    me = lax.axis_index("cls")
    has_west = tile > 0
    has_east = tile < tiles - 1

    barrier = pltpu.get_barrier_semaphore()
    for d in range(1, peers):
        pl.semaphore_signal(
            barrier, inc=1, device_id={"cls": lax.rem(me + d, peers)}, device_id_type=MESH
        )

    @pl.when(has_west)
    def _():
        pl.semaphore_signal(barrier, inc=1, device_id={"tile": tile - 1}, device_id_type=MESH)

    @pl.when(has_east)
    def _():
        pl.semaphore_signal(barrier, inc=1, device_id={"tile": tile + 1}, device_id_type=MESH)

    def packed(l, j):
        return pl.ds(j * layers + l, group, stride=tile_lanes * layers)

    for l in range(layers):
        for j in range(tile_lanes):
            conc_ref[l, :, j * LANES : (j + 1) * LANES] = flat_ref[packed(l, j), :]
    build_tables(levels_ref, target_ref, weights_ref, rate_ref, quad_ref, lin_ref)

    before = lax.div(tile + tiles - 1, tiles)
    after = lax.div(2 * (tiles - 1) - tile, tiles)
    pl.semaphore_wait(barrier, peers - 1 + before + after)

    def cols(x):
        return pl.ds(pl.multiple_of(x * CY, CY), CY)

    def halo(side):
        at = cols(0 if side == 0 else CX - 1)
        to = 1 - side
        where = tile - 1 if side == 0 else tile + 1
        parts = (
            (speed_ref.at[0, :, at], halo_u.at[to]),
            (water_ref.at[:, at], halo_w.at[to]),
            (conc_ref.at[:, :, at], halo_c.at[to]),
        )
        return [
            pltpu.make_async_remote_copy(
                src_ref=part,
                dst_ref=place,
                send_sem=halo_send.at[side, n],
                recv_sem=halo_recv.at[to, n],
                device_id={"tile": where},
                device_id_type=MESH,
            )
            for n, (part, place) in enumerate(parts)
        ]

    def taken(side):
        at = cols(0)
        parts = (
            (speed_ref.at[0, :, at], halo_u.at[side]),
            (water_ref.at[:, at], halo_w.at[side]),
            (conc_ref.at[:, :, at], halo_c.at[side]),
        )
        where = tile - 1 if side == 0 else tile + 1
        return [
            pltpu.make_async_remote_copy(
                src_ref=part,
                dst_ref=place,
                send_sem=halo_send.at[side, n],
                recv_sem=halo_recv.at[side, n],
                device_id={"tile": where},
                device_id_type=MESH,
            )
            for n, (part, place) in enumerate(parts)
        ]

    for side, there in ((0, has_west), (1, has_east)):

        @pl.when(there)
        def _():
            for copy in halo(side):
                copy.start()

        @pl.when(jnp.logical_not(there))
        def _():
            halo_c[side] = jnp.zeros(halo_c.shape[1:], jnp.float32)
            halo_u[side] = jnp.zeros(halo_u.shape[1:], jnp.float32)
            halo_w[side] = jnp.zeros(halo_w.shape[1:], jnp.int32)

    def forward(d, x, s):
        p = lax.rem(me + d, peers)
        return pltpu.make_async_remote_copy(
            src_ref=moved_ref.at[p * own + s, :, cols(x)],
            dst_ref=whole_ref.at[s, pl.ds(pl.multiple_of(me * group, group), group), cols(x)],
            send_sem=out_send.at[d - 1, x, s],
            recv_sem=out_recv.at[d - 1, x, s],
            device_id={"cls": p},
            device_id_type=MESH,
        )

    def backward(d, x, s):
        p = lax.rem(me + d, peers)
        return pltpu.make_async_remote_copy(
            src_ref=done_ref.at[s, pl.ds(pl.multiple_of(p * group, group), group), cols(x)],
            dst_ref=back_ref.at[me * own + s, :, cols(x)],
            send_sem=back_send.at[d - 1, x, s],
            recv_sem=back_recv.at[d - 1, x, s],
            device_id={"cls": p},
            device_id_type=MESH,
        )

    def row_of(x):
        at = cols(x)
        return speed_ref[0, :, at], water_ref[:, at].astype(jnp.float32)

    def halo_row(side):
        return halo_u[side], halo_w[side].astype(jnp.float32)

    square = (group, group)
    diagonal = lax.broadcasted_iota(jnp.int32, square, 0) == lax.broadcasted_iota(
        jnp.int32, square, 1
    )
    settle = jnp.sum(jnp.where(diagonal, settling_ref[...], 0.0), axis=1, keepdims=True)
    settle = jnp.broadcast_to(settle, (group, CY))

    def transport(x):
        at = cols(x)
        u, w = row_of(x)
        u_low, w_low = row_of(x - 1) if x > 0 else halo_row(0)
        u_high, w_high = row_of(x + 1) if x < CX - 1 else halo_row(1)
        face_low = 0.5 * (u_low + u) * (w_low * w)
        face_high = 0.5 * (u + u_high) * (w * w_high)
        v = speed_ref[1, :, at]
        lane = lax.broadcasted_iota(jnp.int32, v.shape, 1)
        w_full = jnp.broadcast_to(w, v.shape)
        side_high = 0.5 * (v + pltpu.roll(v, CY - 1, 1)) * (w_full * pltpu.roll(w_full, CY - 1, 1))
        side_high = jnp.where(lane == CY - 1, 0.0, side_high)
        side_low = pltpu.roll(side_high, 1, 1)
        up = jnp.maximum
        down = jnp.minimum
        centre = (
            1.0 - up(face_high, 0.0) + down(face_low, 0.0) - up(side_high, 0.0) + down(side_low, 0.0)
        )
        west = up(face_low, 0.0)
        east = -down(face_high, 0.0)
        south = up(side_low, 0.0)
        north = -down(side_high, 0.0)
        for l in range(layers):
            c = conc_ref[l, :, at]
            c_west = conc_ref[l, :, cols(x - 1)] if x > 0 else halo_c[0, l]
            c_east = conc_ref[l, :, cols(x + 1)] if x < CX - 1 else halo_c[1, l]
            moved = (
                (centre[l : l + 1] - settle) * c
                + west[l : l + 1] * c_west
                + east[l : l + 1] * c_east
                + south[l : l + 1] * pltpu.roll(c, 1, 1)
                + north[l : l + 1] * pltpu.roll(c, CY - 1, 1)
            )
            if l > 0:
                moved = moved + settle * conc_ref[l - 1, :, at]
            moved_ref[l, :, at] = moved
        for s in range(own):
            whole_ref[s, pl.ds(pl.multiple_of(me * group, group), group), at] = moved_ref[
                me * own + s, :, at
            ]
        for s in range(own):
            for d in range(1, peers):
                forward(d, x, s).start()

    for x in range(1, CX - 1):
        transport(x)
    for side, there, x in ((1, has_east, CX - 1), (0, has_west, 0)):

        @pl.when(there)
        def _():
            for copy in taken(side):
                copy.wait_recv()

        transport(x)

    half = CY // 2

    def react_row(q, carry):
        x = lax.rem(q + 1, CX)
        for s in range(own):
            for d in range(1, peers):
                forward(d, x, s).wait_recv()

            def part(h, carry):
                at = pl.ds(pl.multiple_of(x * CY + h * half, half), half)
                now = react(whole_ref[s, :, at], quad_ref, lin_ref)
                done_ref[s, :, at] = react(now, quad_ref, lin_ref)
                return carry

            lax.fori_loop(0, 2, part, 0)
            back_ref[me * own + s, :, cols(x)] = done_ref[
                s, pl.ds(pl.multiple_of(me * group, group), group), cols(x)
            ]
            for d in range(1, peers):
                backward(d, x, s).start()
        return carry

    lax.fori_loop(0, CX, react_row, 0)

    for side, there in ((0, has_west), (1, has_east)):

        @pl.when(there)
        def _():
            for copy in halo(side):
                copy.wait_send()

    for x in [*range(1, CX), 0]:
        for s in range(own):
            for d in range(1, peers):
                forward(d, x, s).wait_send()
                copy = backward(d, x, s)
                copy.wait_send()
                copy.wait_recv()
        for l in range(layers):
            for j in range(x * CY // LANES, (x + 1) * CY // LANES):
                out_ref[packed(l, j), :] = back_ref[l, :, j * LANES : (j + 1) * LANES]


def body(
    tiles,
    peers,
    concentration,
    velocity,
    land_mask,
    settling,
    breakage_rate,
    kernel_levels,
    pair_target,
    fragment_weights,
):
    group, layers, columns = concentration.shape
    total = kernel_levels.shape[0]
    own = layers // peers
    flat = concentration.reshape(group, layers, columns // LANES, LANES)
    flat = jnp.transpose(flat, (0, 2, 1, 3)).reshape(-1, LANES)
    vmem = pl.BlockSpec(memory_space=pltpu.VMEM)
    dma = pltpu.SemaphoreType.DMA
    done = pl.pallas_call(
        functools.partial(step_kernel, tiles, peers),
        out_shape=jax.ShapeDtypeStruct((group * layers * columns // LANES, LANES), jnp.float32),
        in_specs=[vmem] * 8,
        out_specs=vmem,
        scratch_shapes=[
            pltpu.VMEM((quad_rows(total), 4 * total), jnp.bfloat16),
            pltpu.VMEM((total, 4 * total), jnp.bfloat16),
            pltpu.VMEM((layers, group, columns), jnp.float32),
            pltpu.VMEM((layers, group, columns), jnp.float32),
            pltpu.VMEM((own, total, columns), jnp.float32),
            pltpu.VMEM((own, total, columns), jnp.float32),
            pltpu.VMEM((layers, group, columns), jnp.float32),
            pltpu.VMEM((2, layers, group, CY), jnp.float32),
            pltpu.VMEM((2, layers, CY), jnp.float32),
            pltpu.VMEM((2, 1, CY), jnp.int32),
            dma((2, 3)),
            dma((2, 3)),
            dma((peers - 1, CX, own)),
            dma((peers - 1, CX, own)),
            dma((peers - 1, CX, own)),
            dma((peers - 1, CX, own)),
        ],
        compiler_params=pltpu.CompilerParams(collective_id=0, has_side_effects=True),
    )(
        flat,
        velocity,
        land_mask.reshape(1, columns),
        settling.reshape(1, group),
        breakage_rate.reshape(1, total),
        kernel_levels,
        pair_target,
        fragment_weights,
    )
    done = done.reshape(group, columns // LANES, layers, LANES)
    return jnp.transpose(done, (0, 2, 1, 3)).reshape(group, layers, columns)


def solution(mesh):
    return jax.shard_map(
        functools.partial(body, mesh.shape["tile"], mesh.shape["cls"]),
        mesh=mesh,
        in_specs=(
            P("cls", None, "tile"),
            P(None, None, "tile"),
            P("tile"),
            P("cls"),
            P(),
            P(),
            P(),
            P(),
        ),
        out_specs=P("cls", None, "tile"),
        check_vma=False,
    )
```

```python
import functools

import jax
import jax.numpy as jnp
from jax import lax
from jax.experimental import pallas as pl
from jax.experimental.pallas import tpu as pltpu
from jax.sharding import PartitionSpec as P

CY = 512
CX = 4
half_scale = 0.5e-05
STEP = 8
LANES = 128


def split_pair(value, lane, total):
    high = value.astype(jnp.bfloat16).astype(jnp.float32)
    return jnp.where(lane < total, high, value - high).astype(jnp.bfloat16)


def quad_rows(total):
    return sum(STEP * (total - first) for first in range(0, total, STEP))


def build_tables(levels_ref, target_ref, weights_ref, rate_ref, quad_ref, lin_ref):
    total = levels_ref.shape[0]
    wide = 2 * total
    levels = levels_ref[...].astype(jnp.float32)
    levels = jnp.concatenate([levels, levels], 1)
    target = target_ref[...]
    target = jnp.concatenate([target, target], 1)
    row = lax.broadcasted_iota(jnp.int32, (total, wide), 0)
    lane = lax.broadcasted_iota(jnp.int32, (total, wide), 1)
    col = jnp.where(lane < total, lane, lane - total)
    twice = 2.0 * levels
    birth = jnp.where(col < row, twice, jnp.where(col == row, levels, 0.0))
    offset = 0
    for first in range(0, total, STEP):
        count = total - first
        rank = row[first:]
        for i in range(first, first + STEP):
            value = jnp.where(target[i : i + 1] == rank, birth[i : i + 1], 0.0)
            value = value - jnp.where(rank == i, twice[i : i + 1], 0.0)
            packed = split_pair(value, lane[first:], total)
            quad_ref[offset : offset + count, :wide] = packed
            quad_ref[offset : offset + count, wide:] = packed
            offset += count
    weights = weights_ref[...].astype(jnp.float32)
    weights = jnp.concatenate([weights, weights], 1)
    rate = rate_ref[...]
    rate = jnp.concatenate([rate, rate], 1)
    lower = jnp.where(row <= col, weights, 0.0)
    frag = lower / jnp.sum(lower, axis=0, keepdims=True)
    value = frag * rate - jnp.where(row == col, rate, 0.0)
    packed = split_pair(value, lane, total)
    lin_ref[:, :wide] = packed
    lin_ref[:, wide:] = packed


def react(now, quad_ref, lin_ref):
    total = now.shape[0]
    high = now.astype(jnp.bfloat16)
    low = (now - high.astype(jnp.float32)).astype(jnp.bfloat16)
    stack = jnp.concatenate([high, high, low, low], 0)
    lin = jnp.dot(lin_ref[...], stack, preferred_element_type=jnp.float32)
    gain = None
    offset = 0
    for first in range(0, total, STEP):
        count = total - first
        made = jnp.dot(
            quad_ref[offset : offset + STEP * count, :], stack, preferred_element_type=jnp.float32
        )
        part = made[:count] * now[first : first + 1]
        for r in range(1, STEP):
            part = part + made[r * count : (r + 1) * count] * now[first + r : first + r + 1]
        gain = part if gain is None else jnp.concatenate([gain[:first], gain[first:] + part], 0)
        offset += STEP * count
    return now + gain * half_scale + lin


MESH = pl.DeviceIdType.MESH


def step_kernel(
    tiles,
    peers,
    flat_ref,
    speed_ref,
    water_ref,
    settling_ref,
    rate_ref,
    levels_ref,
    target_ref,
    weights_ref,
    out_ref,
    quad_ref,
    lin_ref,
    conc_ref,
    moved_ref,
    whole_ref,
    done_ref,
    back_ref,
    halo_c,
    halo_u,
    halo_w,
    halo_send,
    halo_recv,
    out_send,
    out_recv,
    back_send,
    back_recv,
):
    layers, group, columns = conc_ref.shape
    tile_lanes = columns // LANES
    own = layers // peers
    tile = lax.axis_index("tile")
    me = lax.axis_index("cls")
    has_west = tile > 0
    has_east = tile < tiles - 1

    barrier = pltpu.get_barrier_semaphore()
    for d in range(1, peers):
        pl.semaphore_signal(
            barrier, inc=1, device_id={"cls": lax.rem(me + d, peers)}, device_id_type=MESH
        )

    @pl.when(has_west)
    def _():
        pl.semaphore_signal(barrier, inc=1, device_id={"tile": tile - 1}, device_id_type=MESH)

    @pl.when(has_east)
    def _():
        pl.semaphore_signal(barrier, inc=1, device_id={"tile": tile + 1}, device_id_type=MESH)

    def packed(l, j):
        return pl.ds(j * layers + l, group, stride=tile_lanes * layers)

    for l in range(layers):
        for j in range(tile_lanes):
            conc_ref[l, :, j * LANES : (j + 1) * LANES] = flat_ref[packed(l, j), :]
    build_tables(levels_ref, target_ref, weights_ref, rate_ref, quad_ref, lin_ref)

    before = lax.div(tile + tiles - 1, tiles)
    after = lax.div(2 * (tiles - 1) - tile, tiles)
    pl.semaphore_wait(barrier, peers - 1 + before + after)

    def cols(x):
        return pl.ds(pl.multiple_of(x * CY, CY), CY)

    def halo(side):
        at = cols(0 if side == 0 else CX - 1)
        to = 1 - side
        where = tile - 1 if side == 0 else tile + 1
        parts = (
            (speed_ref.at[0, :, at], halo_u.at[to]),
            (water_ref.at[:, at], halo_w.at[to]),
            (conc_ref.at[:, :, at], halo_c.at[to]),
        )
        return [
            pltpu.make_async_remote_copy(
                src_ref=part,
                dst_ref=place,
                send_sem=halo_send.at[side, n],
                recv_sem=halo_recv.at[to, n],
                device_id={"tile": where},
                device_id_type=MESH,
            )
            for n, (part, place) in enumerate(parts)
        ]

    def taken(side):
        at = cols(0)
        parts = (
            (speed_ref.at[0, :, at], halo_u.at[side]),
            (water_ref.at[:, at], halo_w.at[side]),
            (conc_ref.at[:, :, at], halo_c.at[side]),
        )
        where = tile - 1 if side == 0 else tile + 1
        return [
            pltpu.make_async_remote_copy(
                src_ref=part,
                dst_ref=place,
                send_sem=halo_send.at[side, n],
                recv_sem=halo_recv.at[side, n],
                device_id={"tile": where},
                device_id_type=MESH,
            )
            for n, (part, place) in enumerate(parts)
        ]

    for side, there in ((0, has_west), (1, has_east)):

        @pl.when(there)
        def _():
            for copy in halo(side):
                copy.start()

        @pl.when(jnp.logical_not(there))
        def _():
            halo_c[side] = jnp.zeros(halo_c.shape[1:], jnp.float32)
            halo_u[side] = jnp.zeros(halo_u.shape[1:], jnp.float32)
            halo_w[side] = jnp.zeros(halo_w.shape[1:], jnp.int32)

    def forward(d, x, s):
        p = lax.rem(me + d, peers)
        return pltpu.make_async_remote_copy(
            src_ref=moved_ref.at[p * own + s, :, cols(x)],
            dst_ref=whole_ref.at[s, pl.ds(pl.multiple_of(me * group, group), group), cols(x)],
            send_sem=out_send.at[d - 1, x, s],
            recv_sem=out_recv.at[d - 1, x, s],
            device_id={"cls": p},
            device_id_type=MESH,
        )

    def backward(d, x, s):
        p = lax.rem(me + d, peers)
        return pltpu.make_async_remote_copy(
            src_ref=done_ref.at[s, pl.ds(pl.multiple_of(p * group, group), group), cols(x)],
            dst_ref=back_ref.at[me * own + s, :, cols(x)],
            send_sem=back_send.at[d - 1, x, s],
            recv_sem=back_recv.at[d - 1, x, s],
            device_id={"cls": p},
            device_id_type=MESH,
        )

    def row_of(x):
        at = cols(x)
        return speed_ref[0, :, at], water_ref[:, at].astype(jnp.float32)

    def halo_row(side):
        return halo_u[side], halo_w[side].astype(jnp.float32)

    square = (group, group)
    diagonal = lax.broadcasted_iota(jnp.int32, square, 0) == lax.broadcasted_iota(
        jnp.int32, square, 1
    )
    settle = jnp.sum(jnp.where(diagonal, settling_ref[...], 0.0), axis=1, keepdims=True)
    settle = jnp.broadcast_to(settle, (group, CY))

    def transport(x):
        at = cols(x)
        u, w = row_of(x)
        u_low, w_low = row_of(x - 1) if x > 0 else halo_row(0)
        u_high, w_high = row_of(x + 1) if x < CX - 1 else halo_row(1)
        face_low = 0.5 * (u_low + u) * (w_low * w)
        face_high = 0.5 * (u + u_high) * (w * w_high)
        v = speed_ref[1, :, at]
        lane = lax.broadcasted_iota(jnp.int32, v.shape, 1)
        w_full = jnp.broadcast_to(w, v.shape)
        side_high = 0.5 * (v + pltpu.roll(v, CY - 1, 1)) * (w_full * pltpu.roll(w_full, CY - 1, 1))
        side_high = jnp.where(lane == CY - 1, 0.0, side_high)
        side_low = pltpu.roll(side_high, 1, 1)
        up = jnp.maximum
        down = jnp.minimum
        centre = (
            1.0 - up(face_high, 0.0) + down(face_low, 0.0) - up(side_high, 0.0) + down(side_low, 0.0)
        )
        west = up(face_low, 0.0)
        east = -down(face_high, 0.0)
        south = up(side_low, 0.0)
        north = -down(side_high, 0.0)
        for l in range(layers):
            c = conc_ref[l, :, at]
            c_west = conc_ref[l, :, cols(x - 1)] if x > 0 else halo_c[0, l]
            c_east = conc_ref[l, :, cols(x + 1)] if x < CX - 1 else halo_c[1, l]
            moved = (
                (centre[l : l + 1] - settle) * c
                + west[l : l + 1] * c_west
                + east[l : l + 1] * c_east
                + south[l : l + 1] * pltpu.roll(c, 1, 1)
                + north[l : l + 1] * pltpu.roll(c, CY - 1, 1)
            )
            if l > 0:
                moved = moved + settle * conc_ref[l - 1, :, at]
            moved_ref[l, :, at] = moved
        for s in range(own):
            whole_ref[s, pl.ds(pl.multiple_of(me * group, group), group), at] = moved_ref[
                me * own + s, :, at
            ]
        for s in range(own):
            for d in range(1, peers):
                forward(d, x, s).start()

    for x in range(1, CX - 1):
        transport(x)
    for side, there, x in ((1, has_east, CX - 1), (0, has_west, 0)):

        @pl.when(there)
        def _():
            for copy in taken(side):
                copy.wait_recv()

        transport(x)

    half = CY

    def react_row(q, carry):
        x = lax.rem(q + 1, CX)
        for s in range(own):
            for d in range(1, peers):
                forward(d, x, s).wait_recv()

            def part(h, carry):
                at = pl.ds(pl.multiple_of(x * CY + h * half, half), half)
                now = react(whole_ref[s, :, at], quad_ref, lin_ref)
                done_ref[s, :, at] = react(now, quad_ref, lin_ref)
                return carry

            part(0, 0)
            back_ref[me * own + s, :, cols(x)] = done_ref[
                s, pl.ds(pl.multiple_of(me * group, group), group), cols(x)
            ]
            for d in range(1, peers):
                backward(d, x, s).start()
        return carry

    lax.fori_loop(0, CX, react_row, 0)

    for side, there in ((0, has_west), (1, has_east)):

        @pl.when(there)
        def _():
            for copy in halo(side):
                copy.wait_send()

    for x in [*range(1, CX), 0]:
        for s in range(own):
            for d in range(1, peers):
                forward(d, x, s).wait_send()
                copy = backward(d, x, s)
                copy.wait_send()
                copy.wait_recv()
        for l in range(layers):
            for j in range(x * CY // LANES, (x + 1) * CY // LANES):
                out_ref[packed(l, j), :] = back_ref[l, :, j * LANES : (j + 1) * LANES]


def body(
    tiles,
    peers,
    concentration,
    velocity,
    land_mask,
    settling,
    breakage_rate,
    kernel_levels,
    pair_target,
    fragment_weights,
):
    group, layers, columns = concentration.shape
    total = kernel_levels.shape[0]
    own = layers // peers
    flat = concentration.reshape(group, layers, columns // LANES, LANES)
    flat = jnp.transpose(flat, (0, 2, 1, 3)).reshape(-1, LANES)
    vmem = pl.BlockSpec(memory_space=pltpu.VMEM)
    dma = pltpu.SemaphoreType.DMA
    done = pl.pallas_call(
        functools.partial(step_kernel, tiles, peers),
        out_shape=pltpu.VMEM((group * layers * columns // LANES, LANES), jnp.float32),
        in_specs=[vmem] * 8,
        out_specs=vmem,
        scratch_shapes=[
            pltpu.VMEM((quad_rows(total), 4 * total), jnp.bfloat16),
            pltpu.VMEM((total, 4 * total), jnp.bfloat16),
            pltpu.VMEM((layers, group, columns), jnp.float32),
            pltpu.VMEM((layers, group, columns), jnp.float32),
            pltpu.VMEM((own, total, columns), jnp.float32),
            pltpu.VMEM((own, total, columns), jnp.float32),
            pltpu.VMEM((layers, group, columns), jnp.float32),
            pltpu.VMEM((2, layers, group, CY), jnp.float32),
            pltpu.VMEM((2, layers, CY), jnp.float32),
            pltpu.VMEM((2, 1, CY), jnp.int32),
            dma((2, 3)),
            dma((2, 3)),
            dma((peers - 1, CX, own)),
            dma((peers - 1, CX, own)),
            dma((peers - 1, CX, own)),
            dma((peers - 1, CX, own)),
        ],
        compiler_params=pltpu.CompilerParams(collective_id=0, has_side_effects=True, vmem_limit_bytes=32 * 1024 * 1024),
    )(
        flat,
        velocity,
        land_mask.reshape(1, columns),
        settling.reshape(1, group),
        breakage_rate.reshape(1, total),
        kernel_levels,
        pair_target,
        fragment_weights,
    )
    done = done.reshape(group, columns // LANES, layers, LANES)
    return jnp.transpose(done, (0, 2, 1, 3)).reshape(group, layers, columns)


def solution(mesh):
    return jax.shard_map(
        functools.partial(body, mesh.shape["tile"], mesh.shape["cls"]),
        mesh=mesh,
        in_specs=(
            P("cls", None, "tile"),
            P(None, None, "tile"),
            P("tile"),
            P("cls"),
            P(),
            P(),
            P(),
            P(),
        ),
        out_specs=P("cls", None, "tile"),
        check_vma=False,
    )
```

```python
import functools

import jax
import jax.numpy as jnp
from jax import lax
from jax.experimental import pallas as pl
from jax.experimental.pallas import tpu as pltpu
from jax.sharding import PartitionSpec as P

CY = 512
CX = 4
half_scale = 0.5e-05
STEP = 8
LANES = 128


def split_pair(value, lane, total):
    high = value.astype(jnp.bfloat16).astype(jnp.float32)
    return jnp.where(lane < total, high, value - high).astype(jnp.bfloat16)


def quad_rows(total):
    return sum(STEP * (total - first) for first in range(0, total, STEP))


def build_tables(levels_ref, target_ref, weights_ref, rate_ref, quad_ref, lin_ref):
    total = levels_ref.shape[0]
    wide = 2 * total
    levels = levels_ref[...].astype(jnp.float32)
    levels = jnp.concatenate([levels, levels], 1)
    target = target_ref[...]
    target = jnp.concatenate([target, target], 1)
    row = lax.broadcasted_iota(jnp.int32, (total, wide), 0)
    lane = lax.broadcasted_iota(jnp.int32, (total, wide), 1)
    col = jnp.where(lane < total, lane, lane - total)
    twice = 2.0 * levels
    birth = jnp.where(col < row, twice, jnp.where(col == row, levels, 0.0))
    offset = 0
    for first in range(0, total, STEP):
        count = total - first
        rank = row[first:]
        for i in range(first, first + STEP):
            value = jnp.where(target[i : i + 1] == rank, birth[i : i + 1], 0.0)
            value = value - jnp.where(rank == i, twice[i : i + 1], 0.0)
            packed = split_pair(value, lane[first:], total)
            quad_ref[offset : offset + count, :wide] = packed
            quad_ref[offset : offset + count, wide:] = packed
            offset += count
    weights = weights_ref[...].astype(jnp.float32)
    weights = jnp.concatenate([weights, weights], 1)
    rate = rate_ref[...]
    rate = jnp.concatenate([rate, rate], 1)
    lower = jnp.where(row <= col, weights, 0.0)
    frag = lower / jnp.sum(lower, axis=0, keepdims=True)
    value = frag * rate - jnp.where(row == col, rate, 0.0)
    packed = split_pair(value, lane, total)
    lin_ref[:, :wide] = packed
    lin_ref[:, wide:] = packed


def react(now, quad_ref, lin_ref):
    total = now.shape[0]
    high = now.astype(jnp.bfloat16)
    low = (now - high.astype(jnp.float32)).astype(jnp.bfloat16)
    stack = jnp.concatenate([high, high, low, low], 0)
    lin = jnp.dot(lin_ref[...], stack, preferred_element_type=jnp.float32)
    gain = None
    offset = 0
    for first in range(0, total, STEP):
        count = total - first
        made = jnp.dot(
            quad_ref[offset : offset + STEP * count, :], stack, preferred_element_type=jnp.float32
        )
        part = made[:count] * now[first : first + 1]
        for r in range(1, STEP):
            part = part + made[r * count : (r + 1) * count] * now[first + r : first + r + 1]
        gain = part if gain is None else jnp.concatenate([gain[:first], gain[first:] + part], 0)
        offset += STEP * count
    return now + gain * half_scale + lin


MESH = pl.DeviceIdType.MESH


def step_kernel(
    tiles,
    peers,
    flat_ref,
    speed_ref,
    water_ref,
    settling_ref,
    rate_ref,
    levels_ref,
    target_ref,
    weights_ref,
    out_ref,
    quad_ref,
    lin_ref,
    conc_ref,
    moved_ref,
    whole_ref,
    done_ref,
    back_ref,
    halo_c,
    halo_u,
    halo_w,
    halo_send,
    halo_recv,
    out_send,
    out_recv,
    back_send,
    back_recv,
):
    layers, group, columns = conc_ref.shape
    tile_lanes = columns // LANES
    own = layers // peers
    tile = lax.axis_index("tile")
    me = lax.axis_index("cls")
    has_west = tile > 0
    has_east = tile < tiles - 1

    barrier = pltpu.get_barrier_semaphore()
    for d in range(1, peers):
        pl.semaphore_signal(
            barrier, inc=1, device_id={"cls": lax.rem(me + d, peers)}, device_id_type=MESH
        )

    @pl.when(has_west)
    def _():
        pl.semaphore_signal(barrier, inc=1, device_id={"tile": tile - 1}, device_id_type=MESH)

    @pl.when(has_east)
    def _():
        pl.semaphore_signal(barrier, inc=1, device_id={"tile": tile + 1}, device_id_type=MESH)

    def packed(l, j):
        return pl.ds(j * layers + l, group, stride=tile_lanes * layers)

    for l in range(layers):
        for j in range(tile_lanes):
            conc_ref[l, :, j * LANES : (j + 1) * LANES] = flat_ref[packed(l, j), :]
    build_tables(levels_ref, target_ref, weights_ref, rate_ref, quad_ref, lin_ref)

    before = lax.div(tile + tiles - 1, tiles)
    after = lax.div(2 * (tiles - 1) - tile, tiles)
    pl.semaphore_wait(barrier, peers - 1 + before + after)

    def cols(x):
        return pl.ds(pl.multiple_of(x * CY, CY), CY)

    def halo(side):
        at = cols(0 if side == 0 else CX - 1)
        to = 1 - side
        where = tile - 1 if side == 0 else tile + 1
        parts = (
            (speed_ref.at[0, :, at], halo_u.at[to]),
            (water_ref.at[:, at], halo_w.at[to]),
            (conc_ref.at[:, :, at], halo_c.at[to]),
        )
        return [
            pltpu.make_async_remote_copy(
                src_ref=part,
                dst_ref=place,
                send_sem=halo_send.at[side, n],
                recv_sem=halo_recv.at[to, n],
                device_id={"tile": where},
                device_id_type=MESH,
            )
            for n, (part, place) in enumerate(parts)
        ]

    def taken(side):
        at = cols(0)
        parts = (
            (speed_ref.at[0, :, at], halo_u.at[side]),
            (water_ref.at[:, at], halo_w.at[side]),
            (conc_ref.at[:, :, at], halo_c.at[side]),
        )
        where = tile - 1 if side == 0 else tile + 1
        return [
            pltpu.make_async_remote_copy(
                src_ref=part,
                dst_ref=place,
                send_sem=halo_send.at[side, n],
                recv_sem=halo_recv.at[side, n],
                device_id={"tile": where},
                device_id_type=MESH,
            )
            for n, (part, place) in enumerate(parts)
        ]

    for side, there in ((0, has_west), (1, has_east)):

        @pl.when(there)
        def _():
            for copy in halo(side):
                copy.start()

        @pl.when(jnp.logical_not(there))
        def _():
            halo_c[side] = jnp.zeros(halo_c.shape[1:], jnp.float32)
            halo_u[side] = jnp.zeros(halo_u.shape[1:], jnp.float32)
            halo_w[side] = jnp.zeros(halo_w.shape[1:], jnp.int32)

    def forward(d, x, s):
        p = lax.rem(me + d, peers)
        return pltpu.make_async_remote_copy(
            src_ref=moved_ref.at[p * own + s, :, cols(x)],
            dst_ref=whole_ref.at[s, pl.ds(pl.multiple_of(me * group, group), group), cols(x)],
            send_sem=out_send.at[d - 1, x, s],
            recv_sem=out_recv.at[d - 1, x, s],
            device_id={"cls": p},
            device_id_type=MESH,
        )

    def backward(d, x, s):
        p = lax.rem(me + d, peers)
        return pltpu.make_async_remote_copy(
            src_ref=done_ref.at[s, pl.ds(pl.multiple_of(p * group, group), group), cols(x)],
            dst_ref=back_ref.at[me * own + s, :, cols(x)],
            send_sem=back_send.at[d - 1, x, s],
            recv_sem=back_recv.at[d - 1, x, s],
            device_id={"cls": p},
            device_id_type=MESH,
        )

    def row_of(x):
        at = cols(x)
        return speed_ref[0, :, at], water_ref[:, at].astype(jnp.float32)

    def halo_row(side):
        return halo_u[side], halo_w[side].astype(jnp.float32)

    square = (group, group)
    diagonal = lax.broadcasted_iota(jnp.int32, square, 0) == lax.broadcasted_iota(
        jnp.int32, square, 1
    )
    settle = jnp.sum(jnp.where(diagonal, settling_ref[...], 0.0), axis=1, keepdims=True)
    settle = jnp.broadcast_to(settle, (group, CY))

    def transport(x):
        at = cols(x)
        u, w = row_of(x)
        u_low, w_low = row_of(x - 1) if x > 0 else halo_row(0)
        u_high, w_high = row_of(x + 1) if x < CX - 1 else halo_row(1)
        face_low = 0.5 * (u_low + u) * (w_low * w)
        face_high = 0.5 * (u + u_high) * (w * w_high)
        v = speed_ref[1, :, at]
        lane = lax.broadcasted_iota(jnp.int32, v.shape, 1)
        w_full = jnp.broadcast_to(w, v.shape)
        side_high = 0.5 * (v + pltpu.roll(v, CY - 1, 1)) * (w_full * pltpu.roll(w_full, CY - 1, 1))
        side_high = jnp.where(lane == CY - 1, 0.0, side_high)
        side_low = pltpu.roll(side_high, 1, 1)
        up = jnp.maximum
        down = jnp.minimum
        centre = (
            1.0 - up(face_high, 0.0) + down(face_low, 0.0) - up(side_high, 0.0) + down(side_low, 0.0)
        )
        west = up(face_low, 0.0)
        east = -down(face_high, 0.0)
        south = up(side_low, 0.0)
        north = -down(side_high, 0.0)
        for l in range(layers):
            c = conc_ref[l, :, at]
            c_west = conc_ref[l, :, cols(x - 1)] if x > 0 else halo_c[0, l]
            c_east = conc_ref[l, :, cols(x + 1)] if x < CX - 1 else halo_c[1, l]
            moved = (
                (centre[l : l + 1] - settle) * c
                + west[l : l + 1] * c_west
                + east[l : l + 1] * c_east
                + south[l : l + 1] * pltpu.roll(c, 1, 1)
                + north[l : l + 1] * pltpu.roll(c, CY - 1, 1)
            )
            if l > 0:
                moved = moved + settle * conc_ref[l - 1, :, at]
            moved_ref[l, :, at] = moved
        for s in range(own):
            whole_ref[s, pl.ds(pl.multiple_of(me * group, group), group), at] = moved_ref[
                me * own + s, :, at
            ]
        for s in range(own):
            for d in range(1, peers):
                forward(d, x, s).start()

    for x in range(1, CX - 1):
        transport(x)
    for side, there, x in ((1, has_east, CX - 1), (0, has_west, 0)):

        @pl.when(there)
        def _():
            for copy in taken(side):
                copy.wait_recv()

        transport(x)

    half = CY

    def react_row(q, carry):
        x = lax.rem(q + 1, CX)
        for s in range(own):
            for d in range(1, peers):
                forward(d, x, s).wait_recv()

            def part(h, carry):
                at = pl.ds(pl.multiple_of(x * CY + h * half, half), half)
                now = react(whole_ref[s, :, at], quad_ref, lin_ref)
                done_ref[s, :, at] = react(now, quad_ref, lin_ref)
                return carry

            part(0, 0)
            back_ref[me * own + s, :, cols(x)] = done_ref[
                s, pl.ds(pl.multiple_of(me * group, group), group), cols(x)
            ]
            for d in range(1, peers):
                backward(d, x, s).start()
        return carry

    lax.fori_loop(0, CX, react_row, 0)

    for side, there in ((0, has_west), (1, has_east)):

        @pl.when(there)
        def _():
            for copy in halo(side):
                copy.wait_send()

    for x in [*range(1, CX), 0]:
        for s in range(own):
            for d in range(1, peers):
                forward(d, x, s).wait_send()
                copy = backward(d, x, s)
                copy.wait_send()
                copy.wait_recv()
        for l in range(layers):
            for j in range(x * CY // LANES, (x + 1) * CY // LANES):
                out_ref[packed(l, j), :] = back_ref[l, :, j * LANES : (j + 1) * LANES]


def body(
    tiles,
    peers,
    concentration,
    velocity,
    land_mask,
    settling,
    breakage_rate,
    kernel_levels,
    pair_target,
    fragment_weights,
):
    group, layers, columns = concentration.shape
    total = kernel_levels.shape[0]
    own = layers // peers
    flat = concentration.reshape(group, layers, columns // LANES, LANES)
    flat = jnp.transpose(flat, (0, 2, 1, 3)).reshape(-1, LANES)
    vmem = pl.BlockSpec(memory_space=pltpu.VMEM)
    dma = pltpu.SemaphoreType.DMA
    done = pl.pallas_call(
        functools.partial(step_kernel, tiles, peers),
        out_shape=pltpu.VMEM((group * layers * columns // LANES, LANES), jnp.float32),
        in_specs=[vmem] * 8,
        out_specs=vmem,
        scratch_shapes=[
            pltpu.VMEM((quad_rows(total), 4 * total), jnp.bfloat16),
            pltpu.VMEM((total, 4 * total), jnp.bfloat16),
            pltpu.VMEM((layers, group, columns), jnp.float32),
            pltpu.VMEM((layers, group, columns), jnp.float32),
            pltpu.VMEM((own, total, columns), jnp.float32),
            pltpu.VMEM((own, total, columns), jnp.float32),
            pltpu.VMEM((layers, group, columns), jnp.float32),
            pltpu.VMEM((2, layers, group, CY), jnp.float32),
            pltpu.VMEM((2, layers, CY), jnp.float32),
            pltpu.VMEM((2, 1, CY), jnp.int32),
            dma((2, 3)),
            dma((2, 3)),
            dma((peers - 1, CX, own)),
            dma((peers - 1, CX, own)),
            dma((peers - 1, CX, own)),
            dma((peers - 1, CX, own)),
        ],
        compiler_params=pltpu.CompilerParams(collective_id=0, has_side_effects=True),
    )(
        flat,
        velocity,
        land_mask.reshape(1, columns),
        settling.reshape(1, group),
        breakage_rate.reshape(1, total),
        kernel_levels,
        pair_target,
        fragment_weights,
    )
    done = done.reshape(group, columns // LANES, layers, LANES)
    return jnp.transpose(done, (0, 2, 1, 3)).reshape(group, layers, columns)


def solution(mesh):
    return jax.shard_map(
        functools.partial(body, mesh.shape["tile"], mesh.shape["cls"]),
        mesh=mesh,
        in_specs=(
            P("cls", None, "tile"),
            P(None, None, "tile"),
            P("tile"),
            P("cls"),
            P(),
            P(),
            P(),
            P(),
        ),
        out_specs=P("cls", None, "tile"),
        check_vma=False,
    )
```
